32 devices in a mesh: dp: 16 (over z, x, core), seq: 2 (over y).
Axes of the slice: x: 2, y: 2, z: 4, core: 2. Of those that a mesh axis runs over, the one named last changes fastest.
Arguments:
- frames: bfloat16 [16, 1024, 512], P('dp', 'seq'), may hold values from -6 to 6
- cotangent: bfloat16 [16, 1024, 512], P('dp', 'seq'), may hold values from -6 to 6
- weight_in: bfloat16 [2, 512, 2176], replicated, may hold values from -0.25 to 0.25
- qk_scales: float32 [2, 2, 128], replicated, may hold values from 0.5 to 1.5
- weight_out: bfloat16 [2, 1024, 512], replicated, may hold values from -0.1875 to 0.1875
- gains: float32 [2, 512], replicated, may hold values from 0.5 to 1.5
Outputs:
- output: bfloat16 [16, 1024, 512], P('dp', 'seq')
- grad_frames: bfloat16 [16, 1024, 512], P('dp', 'seq')
- grad_in: float32 [2, 512, 2176], P(None, 'dp')
- grad_out: float32 [2, 1024, 512], P(None, 'dp')
- grad_gains: float32 [2, 512], replicated
- grad_scales: float32 [2, 2, 128], replicated
The draws below stay inside these ranges and needn't reach their ends.
All inputs are finite; a program needn't handle non-finite values.
Results may differ from the reference program's by a relative error of at most 0.028.
Values may be sent and summed in bfloat16 or wider, within the bound.
No kernel may reach another device: no remote copies, remote signals or barrier semaphores. Data moves between devices by JAX's collectives and lax.ppermute only.
A program may use at most 192 MiB of HBM per device.

```python
from functools import partial
import jax
import jax.numpy as jnp
from jax import lax

D = 512
E = 1024
S = 128
BLOCK = 256
NCH = 4
SEQLEN = 1024
BATCH = 16


def steps_of(own_key, extent, cuts, low, top_value):
    factor_of, own = 1.0, jax.random.fold_in(own_key, 6)
    for axis_at, shards_of in cuts:
        draws = jnp.exp(jax.random.uniform(jax.random.fold_in(own, axis_at), (shards_of,), jnp.float32, low / len(cuts), top_value / len(cuts)))
        factor_of = factor_of * jnp.repeat(draws, extent[axis_at] // shards_of).reshape([-1 if axis == axis_at else 1 for axis in range(len(extent))])
    return factor_of


def bell_draw(key, extent, scale, limit, cuts=(), held_as=jnp.bfloat16):
    entries = scale * jax.random.normal(key, extent, jnp.float32)
    if cuts:
        entries = entries * steps_of(key, extent, cuts, -0.22, 0.18)
    return jnp.clip(entries, -limit, limit).astype(held_as)


def setup_inputs(seed: int = 0) -> dict:
    key_list = jax.random.split(jax.random.key(seed), 7)
    frames = bell_draw(key_list[0], (BATCH, SEQLEN, D), 1.0, 6.0, ((0, 16), (1, 2)))
    cotangent = bell_draw(key_list[1], (BATCH, SEQLEN, D), 1.0, 6.0, ((0, 16), (1, 2)))
    weight_in = bell_draw(key_list[2], (2, D, 2 * E + S), D ** -0.5, 0.25)
    qk_scales = jnp.clip(1.0 + 0.1 * jax.random.normal(key_list[3], (2, 2, S), jnp.float32), 0.5, 1.5)
    weight_out = bell_draw(key_list[4], (2, E, D), E ** -0.5, 0.1875)
    gains = jnp.clip(1.0 + 0.1 * jax.random.normal(key_list[5], (2, D), jnp.float32), 0.5, 1.5)
    return dict(frames=frames, cotangent=cotangent, weight_in=weight_in, qk_scales=qk_scales, weight_out=weight_out, gains=gains)


EPSILON = 1e-06

def normed(values, gain_row):
    scaling = lax.rsqrt(lax.optimization_barrier(jnp.mean(values * values, axis=-1, keepdims=True)) + EPSILON)
    return values * scaling * gain_row

def mixer(projected, scale_pair, attend_axis):
    width = (projected.shape[-1] - scale_pair.shape[-1]) // 2
    active = jax.nn.silu(projected)
    gate_part = active[..., :width]
    value_part = active[..., width:2 * width].astype(jnp.bfloat16)
    shared = active[..., 2 * width:]
    query = (shared * scale_pair[0]).astype(jnp.bfloat16)
    keyed = (shared * scale_pair[1]).astype(jnp.bfloat16)
    length = projected.shape[attend_axis]
    if attend_axis == 1:
        score_form = 'gls,gms->glm'
        mix_form = 'glm,gme->gle'
    else:
        score_form = 'lgs,mgs->glm'
        mix_form = 'glm,mge->lge'
    scores = jnp.einsum(score_form, query.astype(jnp.float32), keyed.astype(jnp.float32))
    scores = scores * scale_pair.shape[-1] ** (-0.5)
    weights = (jnp.square(jax.nn.relu(scores)) / length).astype(jnp.bfloat16)
    mixed = jnp.einsum(mix_form, weights.astype(jnp.float32), value_part.astype(jnp.float32))
    return (gate_part * mixed).astype(jnp.bfloat16)

def rows_product(left, right):
    left_rows = left.reshape(-1, left.shape[-1])
    right_rows = right.reshape(-1, right.shape[-1])
    return lax.dot_general(left_rows, right_rows, (((0,), (0,)), ((), ())), preferred_element_type=jnp.float32)

def against(values, weight):
    return lax.dot_general(values, weight, (((values.ndim - 1,), (1,)), ((), ())), preferred_element_type=jnp.float32)

def unit_forward(inputs_now, weight_in, scale_pair, weight_out, gain_row, attend_axis):
    hidden = normed(inputs_now.astype(jnp.float32), gain_row).astype(jnp.bfloat16)
    projected = jnp.dot(hidden, weight_in, preferred_element_type=jnp.float32)
    gated = mixer(projected, scale_pair, attend_axis)
    result = (inputs_now.astype(jnp.float32) + jnp.dot(gated, weight_out, preferred_element_type=jnp.float32)).astype(jnp.bfloat16)
    return (result, (hidden, projected, gated))

def unit_backward(inputs_now, upstream, weight_in, scale_pair, weight_out, gain_row, saved, attend_axis):
    hidden, projected, gated = saved
    grad_out = rows_product(gated, upstream)
    grad_gated = against(upstream, weight_out).astype(jnp.bfloat16)
    pulled = jax.vjp(partial(mixer, attend_axis=attend_axis), projected, scale_pair)[1]
    grad_proj, grad_scale = pulled(grad_gated)
    grad_proj = grad_proj.astype(jnp.bfloat16)
    grad_in = rows_product(hidden, grad_proj)
    grad_hidden = against(grad_proj, weight_in)
    norm_pull = jax.vjp(normed, inputs_now.astype(jnp.float32), gain_row)[1]
    grad_inputs, grad_gain = norm_pull(grad_hidden)
    grad_inputs = (upstream.astype(jnp.float32) + grad_inputs).astype(jnp.bfloat16)
    return (grad_inputs, grad_in, grad_out, grad_gain, grad_scale)

def reference(frames, cotangent, weight_in, qk_scales, weight_out, gains):
    scaling = (BATCH * SEQLEN) ** (-0.5)

    def one_sequence(carry, pair):
        seq_frames, seq_cot = pair
        blocked = seq_frames.reshape(NCH, BLOCK, D)
        upstream = seq_cot.reshape(NCH, BLOCK, D)
        first, saved_first = unit_forward(blocked, weight_in[0], qk_scales[0], weight_out[0], gains[0], 1)
        second, saved_second = unit_forward(first, weight_in[1], qk_scales[1], weight_out[1], gains[1], 0)
        back_first, in_late, out_late, gain_late, scale_late = unit_backward(first, upstream, weight_in[1], qk_scales[1], weight_out[1], gains[1], saved_second, 0)
        back_frames, in_early, out_early, gain_early, scale_early = unit_backward(blocked, back_first, weight_in[0], qk_scales[0], weight_out[0], gains[0], saved_first, 1)
        carry = (carry[0] + jnp.stack([in_early, in_late]), carry[1] + jnp.stack([out_early, out_late]), carry[2] + jnp.stack([gain_early, gain_late]), carry[3] + jnp.stack([scale_early, scale_late]))
        return (carry, (second.reshape(SEQLEN, D), back_frames.reshape(SEQLEN, D)))
    start = (jnp.zeros((2, D, 2 * E + S), jnp.float32), jnp.zeros((2, E, D), jnp.float32), jnp.zeros((2, D), jnp.float32), jnp.zeros((2, 2, S), jnp.float32))
    totals, outs_pair = lax.scan(one_sequence, start, (frames, cotangent))
    return (outs_pair[0], outs_pair[1], totals[0] * scaling, totals[1] * scaling, totals[2] * scaling, totals[3] * scaling)
```

```python
from functools import partial

import jax
import jax.numpy as jnp
from jax import lax
from jax.sharding import PartitionSpec as P

BLOCK = 256


EPSILON = 1e-06


def normed(values, gain_row):
    scaling = lax.rsqrt(jnp.mean(values * values, axis=-1, keepdims=True) + EPSILON)
    return values * scaling * gain_row


def mixer(projected, scale_pair, attend_axis):
    width = (projected.shape[-1] - scale_pair.shape[-1]) // 2
    active = jax.nn.silu(projected)
    gate_part = active[..., :width]
    value_part = active[..., width : 2 * width].astype(jnp.bfloat16)
    shared = active[..., 2 * width :]
    query = (shared * scale_pair[0]).astype(jnp.bfloat16)
    keyed = (shared * scale_pair[1]).astype(jnp.bfloat16)
    length = projected.shape[attend_axis]
    if attend_axis == 1:
        score_form = "gls,gms->glm"
        mix_form = "glm,gme->gle"
    else:
        score_form = "lgs,mgs->glm"
        mix_form = "glm,mge->lge"
    scores = jnp.einsum(score_form, query, keyed, preferred_element_type=jnp.float32)
    scores = scores * scale_pair.shape[-1] ** (-0.5)
    weights = (jnp.square(jax.nn.relu(scores)) / length).astype(jnp.bfloat16)
    mixed = jnp.einsum(mix_form, weights, value_part, preferred_element_type=jnp.float32)
    return (gate_part * mixed).astype(jnp.bfloat16)


def rows_product(left, right):
    left_rows = left.reshape(-1, left.shape[-1])
    right_rows = right.reshape(-1, right.shape[-1])
    return lax.dot_general(
        left_rows, right_rows, (((0,), (0,)), ((), ())), preferred_element_type=jnp.float32
    )


def against(values, weight):
    return lax.dot_general(
        values, weight, (((values.ndim - 1,), (1,)), ((), ())), preferred_element_type=jnp.float32
    )


def unit_forward(inputs_now, weight_in, scale_pair, weight_out, gain_row, attend_axis):
    hidden = normed(inputs_now.astype(jnp.float32), gain_row).astype(jnp.bfloat16)
    projected = jnp.dot(hidden, weight_in, preferred_element_type=jnp.float32)
    gated = mixer(projected, scale_pair, attend_axis)
    result = (
        inputs_now.astype(jnp.float32)
        + jnp.dot(gated, weight_out, preferred_element_type=jnp.float32)
    ).astype(jnp.bfloat16)
    return (result, (hidden, projected, gated))


def unit_backward(
    inputs_now, upstream, weight_in, scale_pair, weight_out, gain_row, saved, attend_axis
):
    hidden, projected, gated = saved
    grad_out = rows_product(gated, upstream)
    grad_gated = against(upstream, weight_out).astype(jnp.bfloat16)
    pulled = jax.vjp(partial(mixer, attend_axis=attend_axis), projected, scale_pair)[1]
    grad_proj, grad_scale = pulled(grad_gated)
    grad_proj = grad_proj.astype(jnp.bfloat16)
    grad_in = rows_product(hidden, grad_proj)
    grad_hidden = against(grad_proj, weight_in)
    norm_pull = jax.vjp(normed, inputs_now.astype(jnp.float32), gain_row)[1]
    grad_inputs, grad_gain = norm_pull(grad_hidden)
    grad_inputs = (upstream.astype(jnp.float32) + grad_inputs).astype(jnp.bfloat16)
    return (grad_inputs, grad_in, grad_out, grad_gain, grad_scale)


def swapped(values, axis, mask):
    return lax.ppermute(values, axis, [(i, i ^ mask) for i in range(lax.axis_size(axis))])


def bits_of(size):
    count = size.bit_length() - 1
    stages = [(1 << b, (1 << b,)) for b in range(count)]
    if count >= 3:
        low, high = 1 << (count - 2), 1 << (count - 1)
        stages[-2:] = [(low, (low, high)), (low | high, (high,))]
    return stages


def half_of(index, tests):
    total = sum((index // t) % 2 for t in tests)
    return total % 2


def block_order(size, stages):
    return sorted(range(size), key=lambda r: tuple(half_of(r, tests) for _, tests in stages))


def to_slots(values):
    count = lax.axis_size("seq")
    me = lax.axis_index("seq")
    pieces = values.reshape(values.shape[0], count, -1, values.shape[-1])
    return jnp.stack(
        [lax.dynamic_index_in_dim(pieces, me ^ k, 1, keepdims=False) for k in range(count)]
    )


def from_slots(slots):
    count, blocks, _, width = slots.shape
    me = lax.axis_index("seq")
    placed = [lax.dynamic_index_in_dim(slots, me ^ j, 0, keepdims=False) for j in range(count)]
    return jnp.stack(placed, axis=1).reshape(blocks, -1, width)


def exchange(slots):
    return jnp.stack([slots[0]] + [swapped(slots[k], "seq", k) for k in range(1, slots.shape[0])])


def reduced(grad_in, grad_out, scaling, order):
    size = lax.axis_size("dp")
    me = lax.axis_index("dp")
    first, *rest = bits_of(size)
    stages = [first] + rest[order:] + rest[:order]
    rows = grad_in.shape[0] // size
    width = grad_in.shape[1]
    blocks = block_order(size, stages)
    into = (grad_in * scaling).astype(jnp.bfloat16).reshape(size, rows, -1)
    onto = (grad_out * scaling).astype(jnp.bfloat16).reshape(size, -1, rows, grad_out.shape[1])
    current = jnp.stack(
        [jnp.concatenate([into[r]] + [onto[r, k] for k in range(onto.shape[1])], axis=-1) for r in blocks]
    )
    for mask, tests in stages:
        mine = half_of(me, tests)
        halves = current.reshape((2, current.shape[0] // 2) + current.shape[1:])
        away = lax.dynamic_index_in_dim(halves, 1 - mine, 0, keepdims=False)
        kept = lax.dynamic_index_in_dim(halves, mine, 0, keepdims=False)
        came = swapped(away, "dp", mask)
        total = kept.astype(jnp.float32) + came.astype(jnp.float32)
        current = total.astype(jnp.bfloat16)
    for mask, _ in bits_of(lax.axis_size("seq")):
        came = swapped(total.astype(jnp.bfloat16), "seq", mask)
        total = total.astype(jnp.bfloat16).astype(jnp.float32) + came.astype(jnp.float32)
    total = total[0]
    outer = [
        total[:, width + k * grad_out.shape[1] : width + (k + 1) * grad_out.shape[1]]
        for k in range(onto.shape[1])
    ]
    return total[:, :width], jnp.concatenate(outer, axis=0)


def summed_everywhere(values):
    for axis in ("dp", "seq"):
        for mask, _ in bits_of(lax.axis_size(axis)):
            values = values + swapped(values, axis, mask)
    return values


def on_device(frames, cotangent, weight_in, qk_scales, weight_out, gains):
    block_count = frames.shape[1] // BLOCK
    width = frames.shape[2]
    tokens_all = frames.shape[0] * frames.shape[1] * lax.axis_size("dp") * lax.axis_size("seq")
    scaling = tokens_all ** (-0.5)
    upstream = exchange(to_slots(cotangent.reshape(block_count, BLOCK, width)))
    positions = upstream.shape[2]
    upstream = upstream.reshape(-1, positions, width)
    slots_of = lambda v: v.reshape(block_count, -1, positions, width).swapaxes(0, 1)
    blocked = to_slots(frames.reshape(block_count, BLOCK, width)).swapaxes(0, 1)
    blocked = blocked.reshape(block_count, BLOCK, width)
    first, saved_first = unit_forward(
        blocked, weight_in[0], qk_scales[0], weight_out[0], gains[0], 1
    )
    first_pos = exchange(slots_of(first)).reshape(-1, positions, width)
    second, saved_second = unit_forward(
        first_pos, weight_in[1], qk_scales[1], weight_out[1], gains[1], 0
    )
    result = from_slots(exchange(second.reshape(-1, block_count, positions, width)))
    back_pos, in_late, out_late, gain_late, scale_late = unit_backward(
        first_pos, upstream, weight_in[1], qk_scales[1], weight_out[1], gains[1], saved_second, 0
    )
    back_first = exchange(back_pos.reshape(-1, block_count, positions, width))
    back_first = back_first.swapaxes(0, 1).reshape(block_count, BLOCK, width)
    late = reduced(in_late, out_late, scaling, 0)
    back_frames, in_early, out_early, gain_early, scale_early = unit_backward(
        blocked, back_first, weight_in[0], qk_scales[0], weight_out[0], gains[0], saved_first, 1
    )
    early = reduced(in_early, out_early, scaling, 1)
    back_frames = from_slots(slots_of(back_frames))
    small = jnp.concatenate(
        [v.reshape(-1) for v in (gain_early, gain_late, scale_early, scale_late)]
    )
    small = summed_everywhere(small * scaling)
    gain_size = gains.size
    return (
        result.reshape(frames.shape),
        back_frames.reshape(frames.shape),
        jnp.stack([early[0], late[0]]),
        jnp.stack([early[1], late[1]]),
        small[:gain_size].reshape(gains.shape),
        small[gain_size:].reshape(qk_scales.shape),
    )


def solution(mesh):
    in_specs = (P("dp", "seq", None), P("dp", "seq", None), P(), P(), P(), P())
    out_specs = (
        P("dp", "seq", None),
        P("dp", "seq", None),
        P(None, "dp", None),
        P(None, "dp", None),
        P(),
        P(),
    )
    return jax.shard_map(
        on_device, mesh=mesh, in_specs=in_specs, out_specs=out_specs, check_vma=False
    )
```

```python
from functools import partial

import jax
import jax.numpy as jnp
from jax import lax
from jax.experimental import pallas as pl
from jax.experimental.pallas import tpu as pltpu
from jax.sharding import PartitionSpec as P

BLOCK = 256


EPSILON = 1e-06


def sigmoid(values):
    return 0.5 * jnp.tanh(0.5 * values) + 0.5


def slope(values, sig):
    return sig * (1.0 + values * (1.0 - sig))


def dot(left, right, left_dim=1, right_dim=0):
    return lax.dot_general(
        left, right, (((left_dim,), (right_dim,)), ((), ())), preferred_element_type=jnp.float32
    )


def column_chunks(total, size):
    return [(at, min(size, total - at)) for at in range(0, total, size)]


CHUNK = 256


def norm_parts(values):
    scaling = lax.rsqrt(jnp.mean(values * values, axis=-1, keepdims=True) + EPSILON)
    return scaling, values * scaling


def norm_back(values, upstream, grad_hidden, gain_row):
    scaling, unit = norm_parts(values)
    grad_gain = jnp.sum(grad_hidden * unit, axis=0, keepdims=True)
    scaled = grad_hidden * gain_row
    mean = jnp.mean(scaled * unit, axis=-1, keepdims=True)
    return upstream + scaling * (scaled - unit * mean), grad_gain


def group_mask(rows, columns, positions):
    left = lax.broadcasted_iota(jnp.int32, (rows, columns), 0)
    right = lax.broadcasted_iota(jnp.int32, (rows, columns), 1)
    return lax.rem(left, positions) == lax.rem(right, positions)


def scores_of(query, keyed, positions):
    found = jnp.maximum(dot(query, keyed, 1, 1) * query.shape[1] ** (-0.5), 0.0)
    if positions is not None:
        found = jnp.where(group_mask(found.shape[0], found.shape[1], positions), found, 0.0)
    return found


def forward_core(x_ref, h_ref, p_ref, v_ref, o_ref, g_ref, r_ref, win, wout, scales, gain, sets, positions, length):
    half = wout.shape[0]
    values = x_ref[...].astype(jnp.float32)
    h_ref[...] = (norm_parts(values)[1] * gain[...]).astype(jnp.bfloat16)
    shared = dot(h_ref[...], win[:, 2 * half :])
    p_ref[:, 2 * half :] = shared.astype(p_ref.dtype)
    active = shared * sigmoid(shared)
    query = (active * scales[0:1, :]).astype(jnp.bfloat16)
    keyed = (active * scales[1:2, :]).astype(jnp.bfloat16)
    weights = []
    for start, stop in sets:
        found = scores_of(query[start:stop], keyed[start:stop], positions)
        if r_ref is not None:
            r_ref[start:stop, :] = found
        weights.append((found * found * (1.0 / length)).astype(jnp.bfloat16))
    for at, size in column_chunks(half, CHUNK):
        value = dot(h_ref[...], win[:, half + at : half + at + size])
        p_ref[:, half + at : half + at + size] = value.astype(p_ref.dtype)
        v_ref[:, at : at + size] = (value * sigmoid(value)).astype(jnp.bfloat16)
        gate = dot(h_ref[...], win[:, at : at + size])
        p_ref[:, at : at + size] = gate.astype(p_ref.dtype)
        gate = gate * sigmoid(gate)
        for (start, stop), weight in zip(sets, weights):
            mixed = dot(weight, v_ref[start:stop, at : at + size])
            if o_ref is not None:
                o_ref[start:stop, at : at + size] = mixed
            g_ref[start:stop, at : at + size] = (gate[start:stop] * mixed).astype(jnp.bfloat16)
    return values + dot(g_ref[...], wout[...])


def backward_core(dr_ref, p_ref, v_ref, o_ref, g_ref, r_ref, do_ref, dp_ref, wout, scales, sets, positions, length):
    half = wout.shape[0]
    width = scales.shape[1]
    again = o_ref is None
    shared = p_ref[:, 2 * half :].astype(jnp.float32)
    shared_sig = sigmoid(shared)
    active = shared * shared_sig
    query = (active * scales[0:1, :]).astype(jnp.bfloat16)
    keyed = (active * scales[1:2, :]).astype(jnp.bfloat16)
    found, weights = [], []
    for start, stop in sets:
        if again:
            found.append(scores_of(query[start:stop], keyed[start:stop], positions))
        else:
            found.append(r_ref[start:stop, :])
        weights.append((found[-1] * found[-1] * (1.0 / length)).astype(jnp.bfloat16))
    grad_weights = [None for _ in sets]
    for at, size in column_chunks(half, CHUNK):
        here = slice(at, at + size)
        value_here = slice(half + at, half + at + size)
        value = p_ref[:, value_here].astype(jnp.float32)
        value_sig = sigmoid(value)
        if again:
            v_ref[:, here] = (value * value_sig).astype(jnp.bfloat16)
        grad_gated = dot(dr_ref[...], wout[here, :], 1, 1).astype(jnp.bfloat16).astype(jnp.float32)
        gate = p_ref[:, here].astype(jnp.float32)
        gate_sig = sigmoid(gate)
        gated = gate * gate_sig
        do_ref[:, here] = (grad_gated * gated).astype(jnp.bfloat16)
        outer = grad_gated * slope(gate, gate_sig)
        inner = slope(value, value_sig)
        for index, (start, stop) in enumerate(sets):
            if again:
                mixed = dot(weights[index], v_ref[start:stop, here])
                g_ref[start:stop, here] = (gated[start:stop] * mixed).astype(jnp.bfloat16)
            else:
                mixed = o_ref[start:stop, here]
            dp_ref[start:stop, here] = (outer[start:stop] * mixed).astype(jnp.bfloat16)
            grad_value = dot(weights[index], do_ref[start:stop, here], 0, 0)
            grad_value = grad_value.astype(jnp.bfloat16).astype(jnp.float32)
            dp_ref[start:stop, value_here] = (grad_value * inner[start:stop]).astype(jnp.bfloat16)
    totals = [jnp.zeros((1, width), jnp.float32), jnp.zeros((1, width), jnp.float32)]
    for index, (start, stop) in enumerate(sets):
        grad_weight = dot(do_ref[start:stop, :], v_ref[start:stop, :], 1, 1)
        grad_weight = grad_weight.astype(jnp.bfloat16).astype(jnp.float32)
        grad_score = grad_weight * found[index] * (2.0 / length * width ** (-0.5))
        if positions is not None:
            grad_score = jnp.where(
                group_mask(grad_score.shape[0], grad_score.shape[1], positions), grad_score, 0.0
            )
        grad_score = grad_score.astype(jnp.bfloat16)
        part = active[start:stop]
        grad_query = dot(grad_score, keyed[start:stop]).astype(jnp.bfloat16).astype(jnp.float32)
        grad_keyed = dot(grad_score, query[start:stop], 0, 0).astype(jnp.bfloat16).astype(jnp.float32)
        totals[0] += jnp.sum(grad_query * part, axis=0, keepdims=True)
        totals[1] += jnp.sum(grad_keyed * part, axis=0, keepdims=True)
        grad_shared = grad_query * scales[0:1, :] + grad_keyed * scales[1:2, :]
        grad_shared = grad_shared * slope(shared[start:stop], shared_sig[start:stop])
        dp_ref[start:stop, 2 * half :] = grad_shared.astype(jnp.bfloat16)
    return totals


def first_kernel(shape, me_ref, frames, win, wout, scales, gain, first, h_ref, p_ref, x_ref, v_ref, g_ref):
    slots, blocks, positions = shape
    me = me_ref[0]
    size = slots * positions
    for b in range(blocks):
        for k in range(slots):
            at = pl.multiple_of((me ^ k) * positions, positions)
            x_ref[b * size + k * positions : b * size + (k + 1) * positions, :] = frames[b, pl.ds(at, positions), :]
    sets = [(b * size, (b + 1) * size) for b in range(blocks)]
    result = forward_core(
        x_ref, h_ref, p_ref, v_ref, None, g_ref, None, win, wout, scales, gain, sets, None, size
    ).astype(jnp.bfloat16)
    for b in range(blocks):
        for k in range(slots):
            first[k, b] = result[b * size + k * positions : b * size + (k + 1) * positions]


def second_kernel(
    shape, length, x_ref, dr_ref, win, wout, scales, gain,
    second, back, h_ref, dp_ref, g_ref, dgain, dscales, p_ref, v_ref, o_ref, r_ref, do_ref,
):
    positions = shape[2]
    sets = [(0, x_ref.shape[0])]
    second[...] = forward_core(
        x_ref, h_ref, p_ref, v_ref, o_ref, g_ref, r_ref, win, wout, scales, gain, sets, positions, length
    ).astype(jnp.bfloat16)
    totals = backward_core(
        dr_ref, p_ref, v_ref, o_ref, g_ref, r_ref, do_ref, dp_ref, wout, scales, sets, positions, length
    )
    dscales[0:1, :] = totals[0]
    dscales[1:2, :] = totals[1]
    grad_hidden = dot(dp_ref[...], win[...], 1, 1)
    result, dgain[...] = norm_back(
        x_ref[...].astype(jnp.float32), dr_ref[...].astype(jnp.float32), grad_hidden, gain[...]
    )
    back[...] = result.astype(jnp.bfloat16)


def third_kernel(shape, slots_ref, p_ref, wout, scales, dr_ref, dp_ref, g_ref, dscales, v_ref, do_ref):
    slots, blocks, positions = shape
    size = slots * positions
    for b in range(blocks):
        for k in range(slots):
            dr_ref[b * size + k * positions : b * size + (k + 1) * positions, :] = slots_ref[k, b]
    sets = [(b * size, (b + 1) * size) for b in range(blocks)]
    totals = backward_core(
        dr_ref, p_ref, v_ref, None, g_ref, None, do_ref, dp_ref, wout, scales, sets, None, size
    )
    dscales[0:1, :] = totals[0]
    dscales[1:2, :] = totals[1]


def fourth_kernel(shape, me_ref, frames, dr_ref, dp_ref, win, gain, grad_frames, dgain, x_ref):
    slots, blocks, positions = shape
    me = me_ref[0]
    size = slots * positions
    for b in range(blocks):
        for k in range(slots):
            at = pl.multiple_of((me ^ k) * positions, positions)
            x_ref[b * size + k * positions : b * size + (k + 1) * positions, :] = frames[b, pl.ds(at, positions), :]
    grad_hidden = dot(dp_ref[...], win[...], 1, 1)
    result, dgain[...] = norm_back(
        x_ref[...].astype(jnp.float32), dr_ref[...].astype(jnp.float32), grad_hidden, gain[...]
    )
    result = result.astype(jnp.bfloat16)
    for b in range(blocks):
        for k in range(slots):
            at = pl.multiple_of((me ^ k) * positions, positions)
            grad_frames[b, pl.ds(at, positions), :] = result[b * size + k * positions : b * size + (k + 1) * positions]


def weights_kernel(plan, scaling, h_ref, dp_ref, g_ref, dr_ref, *outs):
    shards = outs[0].shape[0]
    rows = outs[0].shape[1]
    width = dp_ref.shape[1]
    for out, (start, stop, blocks) in zip(outs, plan):
        low, high = start, min(stop, width)
        for at, size in column_chunks(max(high - low, 0), 512):
            found = dot(h_ref[...], dp_ref[:, low + at : low + at + size], 0, 0) * scaling
            found = found.astype(jnp.bfloat16)
            for place, r in enumerate(blocks):
                out[place, :, low + at - start : low + at - start + size] = found[r * rows : (r + 1) * rows]
    per = dr_ref.shape[1]
    found = (dot(g_ref[...], dr_ref[...], 0, 0) * scaling).astype(jnp.bfloat16)
    pieces = found.shape[0] // (shards * rows)
    for out, (start, stop, blocks) in zip(outs, plan):
        for k in range(pieces):
            low, high = max(start, width + k * per), min(stop, width + (k + 1) * per)
            if low >= high:
                continue
            for place, r in enumerate(blocks):
                top = (r * pieces + k) * rows
                out[place, :, low - start : high - start] = found[top : top + rows, low - width - k * per : high - width - k * per]


VMEM = pltpu.MemorySpace.VMEM
SMEM = pltpu.MemorySpace.SMEM
LIMIT = 48 * 2**20


class Fetched:
    def __init__(self, source, unit, target, semaphore):
        self.copy = pltpu.make_async_copy(source.at[unit], target, semaphore)
        self.copy.start()
        self.target = target
        self.shape = target.shape
        self.landed = False

    def __getitem__(self, index):
        if not self.landed:
            self.copy.wait()
            self.landed = True
        return self.target[index]


def run(name, body, ins, outs, scratch, flops, smem=0):
    specs = [pl.BlockSpec(memory_space=SMEM if i < smem else VMEM) for i in range(len(ins))]
    fetched = [i for i, v in enumerate(ins) if isinstance(v, tuple)]
    for i in fetched:
        specs[i] = pl.BlockSpec(memory_space=pl.ANY)
    targets = [pltpu.VMEM(ins[i][0].shape[1:], ins[i][0].dtype) for i in fetched]

    def kernel(*refs):
        refs = list(refs)
        spare = refs[len(refs) - len(fetched) - 1 :] if fetched else []
        refs = refs[: len(refs) - len(spare)]
        for k, i in enumerate(fetched):
            refs[i] = Fetched(refs[i], ins[i][1], spare[k], spare[-1].at[k])
        body(*refs)

    return pl.pallas_call(
        kernel,
        out_shape=[jax.ShapeDtypeStruct(s, d) for s, d in outs],
        in_specs=specs,
        out_specs=[pl.BlockSpec(memory_space=VMEM) for _ in outs],
        scratch_shapes=[pltpu.VMEM(s, d) for s, d in scratch]
        + targets
        + ([pltpu.SemaphoreType.DMA((len(fetched),))] if fetched else []),
        compiler_params=pltpu.CompilerParams(vmem_limit_bytes=LIMIT),
        cost_estimate=pl.CostEstimate(flops=flops, bytes_accessed=2**22, transcendentals=0),
        name=name,
    )(*[v[0] if isinstance(v, tuple) else v for v in ins])


def swapped(values, axis, mask):
    return lax.ppermute(values, axis, [(i, i ^ mask) for i in range(lax.axis_size(axis))])


def bits_of(size):
    count = size.bit_length() - 1
    stages = [(1 << b, (1 << b,)) for b in range(count)]
    if count >= 3:
        low, high = 1 << (count - 2), 1 << (count - 1)
        stages[-2:] = [(low, (low, high)), (low | high, (high,))]
    return stages


def half_of(index, tests):
    total = sum((index // t) % 2 for t in tests)
    return total % 2


def block_order(size, stages):
    return sorted(range(size), key=lambda r: tuple(half_of(r, tests) for _, tests in stages))


def slots_from(values):
    count = lax.axis_size("seq")
    me = lax.axis_index("seq")
    pieces = values.reshape(values.shape[0], count, -1, values.shape[-1])
    return [lax.dynamic_index_in_dim(pieces, me ^ k, 1, keepdims=False) for k in range(count)]


def from_slots(slots):
    count, blocks, _, width = slots.shape
    me = lax.axis_index("seq")
    placed = [lax.dynamic_index_in_dim(slots, me ^ j, 0, keepdims=False) for j in range(count)]
    return jnp.stack(placed, axis=1).reshape(blocks, -1, width)


def rotated(stages, turn):
    first, *rest = stages
    turn %= max(len(rest), 1)
    return [first] + rest[turn:] + rest[:turn]


def halved(current, mine):
    halves = current.reshape((2, current.shape[0] // 2) + current.shape[1:])
    away = lax.dynamic_index_in_dim(halves, 1 - mine, 0, keepdims=False)
    kept = lax.dynamic_index_in_dim(halves, mine, 0, keepdims=False)
    return away, kept


class Chain:
    def __init__(self, current, turn):
        self.stages = rotated(bits_of(lax.axis_size("dp")), turn)
        self.extra = list(bits_of(lax.axis_size("seq")))
        self.current = current
        self.at = 0
        self.prepare()

    def prepare(self):
        if self.at < len(self.stages):
            mine = half_of(lax.axis_index("dp"), self.stages[self.at][1])
            self.away, self.kept = halved(self.current, mine)
        else:
            self.away = self.kept = self.current

    def send(self):
        if self.at < len(self.stages):
            self.came = swapped(self.away, "dp", self.stages[self.at][0])
        else:
            self.came = swapped(self.away, "seq", self.extra[self.at - len(self.stages)][0])

    def land(self):
        total = self.kept.astype(jnp.float32) + self.came.astype(jnp.float32)
        self.at += 1
        if self.done():
            self.total = total[0]
        else:
            self.current = total.astype(jnp.bfloat16)
            self.prepare()

    def done(self):
        return self.at == len(self.stages) + len(self.extra)

    def finish(self):
        while not self.done():
            self.send()
            self.land()
        return self.total


def unpacked(total, width, out_width):
    outer = [
        total[:, at : at + out_width] for at in range(width, total.shape[1], out_width)
    ]
    return total[:, :width], jnp.concatenate(outer, axis=0)


def summed_everywhere(values):
    for axis in ("dp", "seq"):
        for mask, _ in bits_of(lax.axis_size(axis)):
            values = values + swapped(values, axis, mask)
    return values


LATE = (1,)
EARLY = (0, 1)


def plan_of(width, turns):
    size = lax.axis_size("dp")
    edges = [width * k // len(turns) // 128 * 128 for k in range(len(turns))] + [width]
    orders = [block_order(size, rotated(bits_of(size), turn)) for turn in turns]
    return [(edges[k], edges[k + 1], orders[k]) for k in range(len(turns))]


def unit_chains(name, turns, scaling, hidden, grad_proj, gated, grad_result):
    size = lax.axis_size("dp")
    rows = hidden.shape[1] // size
    width = grad_proj.shape[1] + gated.shape[1] * grad_result.shape[1] // (size * rows)
    plan = plan_of(width, turns)
    buffers = run(
        name,
        partial(weights_kernel, plan, scaling),
        [hidden, grad_proj, gated, grad_result],
        [((size, rows, stop - start), jnp.bfloat16) for start, stop, _ in plan],
        [],
        2 * hidden.shape[0] * size * rows * width,
    )
    return [Chain(buffer, turn) for buffer, turn in zip(buffers, turns)]


def tied(*values):
    return lax.optimization_barrier(values)


def on_device(frames, cotangent, weight_in, qk_scales, weight_out, gains):
    slots = lax.axis_size("seq")
    blocks = frames.shape[1] // BLOCK
    positions = BLOCK // slots
    shape = (slots, blocks, positions)
    count, width = frames.shape[1:]
    inner, half, shared = weight_in.shape[2], weight_out.shape[1], qk_scales.shape[2]
    tokens_all = frames.shape[0] * count * lax.axis_size("dp") * slots
    scaling = tokens_all ** (-0.5)
    me = lax.axis_index("seq").astype(jnp.int32).reshape(1)
    flops = 2 * count * width * inner
    bf16, f32 = jnp.bfloat16, jnp.float32
    blocked = frames.reshape(blocks, BLOCK, width)

    def exchange(slot_list):
        return jnp.stack([slot_list[0]] + [swapped(slot_list[k], "seq", k) for k in range(1, slots)])

    upstream = exchange(slots_from(cotangent.reshape(blocks, BLOCK, width)))
    upstream = upstream.reshape(count, width)
    first, hidden_first, proj_first = run(
        "first",
        lambda me, x, wi, wo, sc, ga, *rest: first_kernel(shape, me, x, wi, wo, sc.at[0], ga.at[0:1], *rest),
        [me, blocked, (weight_in, 0), (weight_out, 0), qk_scales, gains],
        [((slots, blocks, positions, width), bf16), ((count, width), bf16), ((count, inner), bf16)],
        [((count, width), bf16), ((count, half), bf16), ((count, half), bf16)],
        2 * flops,
        smem=1,
    )
    first_pos = exchange(first).reshape(count, width)
    second, back_pos, hidden_second, dproj_second, gated_second, dgain_late, dscale_late = run(
        "second",
        lambda x, dr, wi, wo, sc, ga, *rest: second_kernel(
            shape, slots * blocks, x, dr, wi, wo, sc.at[1], ga.at[1:2], *rest
        ),
        [first_pos, upstream, (weight_in, 1), (weight_out, 1), qk_scales, gains],
        [
            ((count, width), bf16),
            ((count, width), bf16),
            ((count, width), bf16),
            ((count, inner), bf16),
            ((count, half), bf16),
            ((1, width), f32),
            ((2, shared), f32),
        ],
        [((count, inner), f32), ((count, half), bf16), ((count, half), f32), ((count, count), f32), ((count, half), bf16)],
        4 * flops,
    )
    slotted = (slots, blocks, positions, width)
    back_first = exchange(back_pos.reshape(slotted))
    late = unit_chains("late", LATE, scaling, hidden_second, dproj_second, gated_second, upstream)
    for chain in late:
        chain.send()
        chain.land()
    back_first, second, *aways = tied(back_first, second, *[c.away for c in late])
    for chain, away in zip(late, aways):
        chain.away = away
        chain.send()
    dresult, dproj_first, gated_first, dscale_early = run(
        "third",
        lambda dr, p, wo, sc, *rest: third_kernel(shape, dr, p, wo, sc.at[0], *rest),
        [back_first, proj_first, (weight_out, 0), qk_scales],
        [((count, width), bf16), ((count, inner), bf16), ((count, half), bf16), ((2, shared), f32)],
        [((count, half), bf16), ((count, half), bf16)],
        2 * flops,
    )
    early = unit_chains("early", EARLY, scaling, hidden_first, dproj_first, gated_first, dresult)
    back_frames, dgain_early = run(
        "fourth",
        lambda me, x, dr, dp, wi, ga, *rest: fourth_kernel(shape, me, x, dr, dp, wi, ga.at[0:1], *rest),
        [me, blocked, dresult, dproj_first, (weight_in, 0), gains],
        [((blocks, BLOCK, width), bf16), ((1, width), f32)],
        [((count, width), bf16)],
        flops,
        smem=1,
    )
    small = jnp.concatenate(
        [v.reshape(-1) for v in (dgain_early, dgain_late, dscale_early, dscale_late)]
    ) * scaling
    for chain in early:
        chain.send()
    for chain in late:
        chain.land()
    for chain in early:
        chain.land()
    masks = [(a, m) for a in ("dp", "seq") for m, _ in bits_of(lax.axis_size(a))]
    result = None
    while not all(c.done() for c in early) or masks:
        live = [c for c in early + late if not c.done()]
        if masks:
            small, second, back_frames, *aways = tied(
                small, second, back_frames, *[c.away for c in live]
            )
        else:
            aways = tied(*[c.away for c in live])
        for chain, away in zip(live, aways):
            chain.away = away
            chain.send()
        if masks:
            axis, mask = masks.pop(0)
            small = small + swapped(small, axis, mask)
        if result is None:
            result = from_slots(exchange(second.reshape(slotted)))
        for chain in live:
            chain.land()
    shards = [
        unpacked(jnp.concatenate([c.finish() for c in chains], axis=-1), inner, width)
        for chains in (early, late)
    ]
    gain_size = gains.size
    return (
        result.reshape(frames.shape),
        back_frames.reshape(frames.shape),
        jnp.stack([shards[0][0], shards[1][0]]),
        jnp.stack([shards[0][1], shards[1][1]]),
        small[:gain_size].reshape(gains.shape),
        small[gain_size:].reshape(qk_scales.shape),
    )


def solution(mesh):
    in_specs = (P("dp", "seq", None), P("dp", "seq", None), P(), P(), P(), P())
    out_specs = (
        P("dp", "seq", None),
        P("dp", "seq", None),
        P(None, "dp", None),
        P(None, "dp", None),
        P(),
        P(),
    )
    return jax.shard_map(
        on_device, mesh=mesh, in_specs=in_specs, out_specs=out_specs, check_vma=False
    )
```

```python
from functools import partial

import jax
import jax.numpy as jnp
from jax import lax
from jax.experimental import pallas as pl
from jax.experimental.pallas import tpu as pltpu
from jax.sharding import PartitionSpec as P


BLOCK = 256


EPSILON = 1e-06


def sigmoid(values):
    return 0.5 * jnp.tanh(0.5 * values) + 0.5


def slope(values, sig):
    return sig * (1.0 + values * (1.0 - sig))


def dot(left, right, left_dim=1, right_dim=0):
    return lax.dot_general(
        left, right, (((left_dim,), (right_dim,)), ((), ())), preferred_element_type=jnp.float32
    )


def column_chunks(total, size):
    return [(at, min(size, total - at)) for at in range(0, total, size)]


CHUNK = 256


def norm_parts(values):
    scaling = lax.rsqrt(jnp.mean(values * values, axis=-1, keepdims=True) + EPSILON)
    return scaling, values * scaling


def norm_back(values, upstream, grad_hidden, gain_row):
    scaling, unit = norm_parts(values)
    grad_gain = jnp.sum(grad_hidden * unit, axis=0, keepdims=True)
    scaled = grad_hidden * gain_row
    mean = jnp.mean(scaled * unit, axis=-1, keepdims=True)
    return upstream + scaling * (scaled - unit * mean), grad_gain


def group_mask(rows, columns, positions):
    left = lax.broadcasted_iota(jnp.int32, (rows, columns), 0)
    right = lax.broadcasted_iota(jnp.int32, (rows, columns), 1)
    return lax.rem(left, positions) == lax.rem(right, positions)


def scores_of(query, keyed, positions):
    found = jnp.maximum(dot(query, keyed, 1, 1) * query.shape[1] ** (-0.5), 0.0)
    if positions is not None:
        found = jnp.where(group_mask(found.shape[0], found.shape[1], positions), found, 0.0)
    return found


def forward_core(x_ref, h_ref, p_ref, v_ref, o_ref, g_ref, r_ref, win, wout, scales, gain, sets, positions, length):
    half = wout.shape[0]
    values = x_ref[...].astype(jnp.float32)
    h_ref[...] = (norm_parts(values)[1] * gain[...]).astype(jnp.bfloat16)
    shared = dot(h_ref[...], win[:, 2 * half :])
    p_ref[:, 2 * half :] = shared.astype(p_ref.dtype)
    active = shared * sigmoid(shared)
    query = (active * scales[0:1, :]).astype(jnp.bfloat16)
    keyed = (active * scales[1:2, :]).astype(jnp.bfloat16)
    weights = []
    for start, stop in sets:
        found = scores_of(query[start:stop], keyed[start:stop], positions)
        if r_ref is not None:
            r_ref[start:stop, :] = found
        weights.append((found * found * (1.0 / length)).astype(jnp.bfloat16))
    for at, size in column_chunks(half, CHUNK):
        value = dot(h_ref[...], win[:, half + at : half + at + size])
        p_ref[:, half + at : half + at + size] = value.astype(p_ref.dtype)
        v_ref[:, at : at + size] = (value * sigmoid(value)).astype(jnp.bfloat16)
        gate = dot(h_ref[...], win[:, at : at + size])
        p_ref[:, at : at + size] = gate.astype(p_ref.dtype)
        gate = gate * sigmoid(gate)
        for (start, stop), weight in zip(sets, weights):
            mixed = dot(weight, v_ref[start:stop, at : at + size])
            if o_ref is not None:
                o_ref[start:stop, at : at + size] = mixed
            g_ref[start:stop, at : at + size] = (gate[start:stop] * mixed).astype(jnp.bfloat16)
    return values + dot(g_ref[...], wout[...])


def backward_core(dr_ref, p_ref, v_ref, o_ref, g_ref, r_ref, do_ref, dp_ref, wout, scales, sets, positions, length):
    half = wout.shape[0]
    width = scales.shape[1]
    again = o_ref is None
    shared = p_ref[:, 2 * half :].astype(jnp.float32)
    shared_sig = sigmoid(shared)
    active = shared * shared_sig
    query = (active * scales[0:1, :]).astype(jnp.bfloat16)
    keyed = (active * scales[1:2, :]).astype(jnp.bfloat16)
    found, weights = [], []
    for start, stop in sets:
        if again:
            found.append(scores_of(query[start:stop], keyed[start:stop], positions))
        else:
            found.append(r_ref[start:stop, :])
        weights.append((found[-1] * found[-1] * (1.0 / length)).astype(jnp.bfloat16))
    grad_weights = [None for _ in sets]
    for at, size in column_chunks(half, CHUNK):
        here = slice(at, at + size)
        value_here = slice(half + at, half + at + size)
        value = p_ref[:, value_here].astype(jnp.float32)
        value_sig = sigmoid(value)
        if again:
            v_ref[:, here] = (value * value_sig).astype(jnp.bfloat16)
        grad_gated = dot(dr_ref[...], wout[here, :], 1, 1).astype(jnp.bfloat16).astype(jnp.float32)
        gate = p_ref[:, here].astype(jnp.float32)
        gate_sig = sigmoid(gate)
        gated = gate * gate_sig
        do_ref[:, here] = (grad_gated * gated).astype(jnp.bfloat16)
        outer = grad_gated * slope(gate, gate_sig)
        inner = slope(value, value_sig)
        for index, (start, stop) in enumerate(sets):
            if again:
                mixed = dot(weights[index], v_ref[start:stop, here])
                g_ref[start:stop, here] = (gated[start:stop] * mixed).astype(jnp.bfloat16)
            else:
                mixed = o_ref[start:stop, here]
            dp_ref[start:stop, here] = (outer[start:stop] * mixed).astype(jnp.bfloat16)
            grad_value = dot(weights[index], do_ref[start:stop, here], 0, 0)
            grad_value = grad_value.astype(jnp.bfloat16).astype(jnp.float32)
            dp_ref[start:stop, value_here] = (grad_value * inner[start:stop]).astype(jnp.bfloat16)
    totals = [jnp.zeros((1, width), jnp.float32), jnp.zeros((1, width), jnp.float32)]
    for index, (start, stop) in enumerate(sets):
        grad_weight = dot(do_ref[start:stop, :], v_ref[start:stop, :], 1, 1)
        grad_weight = grad_weight.astype(jnp.bfloat16).astype(jnp.float32)
        grad_score = grad_weight * found[index] * (2.0 / length * width ** (-0.5))
        if positions is not None:
            grad_score = jnp.where(
                group_mask(grad_score.shape[0], grad_score.shape[1], positions), grad_score, 0.0
            )
        grad_score = grad_score.astype(jnp.bfloat16)
        part = active[start:stop]
        grad_query = dot(grad_score, keyed[start:stop]).astype(jnp.bfloat16).astype(jnp.float32)
        grad_keyed = dot(grad_score, query[start:stop], 0, 0).astype(jnp.bfloat16).astype(jnp.float32)
        totals[0] += jnp.sum(grad_query * part, axis=0, keepdims=True)
        totals[1] += jnp.sum(grad_keyed * part, axis=0, keepdims=True)
        grad_shared = grad_query * scales[0:1, :] + grad_keyed * scales[1:2, :]
        grad_shared = grad_shared * slope(shared[start:stop], shared_sig[start:stop])
        dp_ref[start:stop, 2 * half :] = grad_shared.astype(jnp.bfloat16)
    return totals


def copy_blocks(shape, me, source, target):
    slots, blocks, positions = shape
    size = slots * positions
    for b in range(blocks):
        for k in range(slots):
            at = pl.multiple_of((me ^ k) * positions, positions)
            target[b * size + k * positions : b * size + (k + 1) * positions, :] = source[b, pl.ds(at, positions), :]


def first_kernel(shape, me_ref, frames, win, wout, scales, gain, *rest):
    slots, blocks, positions = shape
    sends, (h_ref, p_ref, x_ref, v_ref, g_ref) = rest[:slots], rest[slots:]
    size = slots * positions
    copy_blocks(shape, me_ref[0], frames.now(), x_ref)
    sets = [(b * size, (b + 1) * size) for b in range(blocks)]
    result = forward_core(
        x_ref, h_ref, p_ref, v_ref, None, g_ref, None, win, wout, scales, gain, sets, None, size
    ).astype(jnp.bfloat16)
    for b in range(blocks):
        for k in range(slots):
            sends[k][b * positions : (b + 1) * positions, :] = result[b * size + k * positions : b * size + (k + 1) * positions]


def second_kernel(shape, length, scaling, me_ref, cotangent, win, wout, scales, gain, *rest):
    slots, blocks, positions = shape
    part = blocks * positions
    xs, drs, rest = rest[:slots], rest[slots : 2 * slots - 1], rest[2 * slots - 1 :]
    seconds, backs, rest = rest[:slots], rest[slots : 2 * slots], rest[2 * slots :]
    h_ref, dp_ref, g_ref, dr_ref, small, x_ref, p_ref, v_ref, o_ref, r_ref, do_ref = rest
    at = pl.multiple_of(me_ref[0] * positions, positions)
    for k in range(slots):
        x_ref[k * part : (k + 1) * part, :] = xs[k][...]
        if k:
            dr_ref[k * part : (k + 1) * part, :] = drs[k - 1][...]
    for b in range(blocks):
        dr_ref[b * positions : (b + 1) * positions, :] = cotangent.now()[b, pl.ds(at, positions), :]
    sets = [(0, x_ref.shape[0])]
    result = forward_core(
        x_ref, h_ref, p_ref, v_ref, o_ref, g_ref, r_ref, win, wout, scales, gain, sets, positions, length
    ).astype(jnp.bfloat16)
    for k in range(slots):
        seconds[k][...] = result[k * part : (k + 1) * part]
    totals = backward_core(
        dr_ref, p_ref, v_ref, o_ref, g_ref, r_ref, do_ref, dp_ref, wout, scales, sets, positions, length
    )
    grad_hidden = dot(dp_ref[...], win[...], 1, 1)
    result, grad_gain = norm_back(
        x_ref[...].astype(jnp.float32), dr_ref[...].astype(jnp.float32), grad_hidden, gain[...]
    )
    result = result.astype(jnp.bfloat16)
    for k in range(slots):
        backs[k][...] = result[k * part : (k + 1) * part]
    fill_small(small, 0, scaling, [grad_gain] + totals)


def fill_small(small, start, scaling, values):
    row = start
    for value in values:
        for at in range(0, value.shape[1], 128):
            small[row : row + 1, :] = value[:, at : at + 128] * scaling
            row += 1
    while row % 8:
        small[row : row + 1, :] = jnp.zeros((1, 128), jnp.float32)
        row += 1


def third_kernel(shape, wout, scales, *rest):
    slots, blocks, positions = shape
    size = slots * positions
    slot_refs, (p_ref, dr_ref, dp_ref, g_ref, dscales, v_ref, do_ref) = rest[:slots], rest[slots:]
    for b in range(blocks):
        for k in range(slots):
            dr_ref[b * size + k * positions : b * size + (k + 1) * positions, :] = slot_refs[k][b * positions : (b + 1) * positions, :]
    sets = [(b * size, (b + 1) * size) for b in range(blocks)]
    totals = backward_core(
        dr_ref, p_ref, v_ref, None, g_ref, None, do_ref, dp_ref, wout, scales, sets, None, size
    )
    dscales[0:1, :] = totals[0]
    dscales[1:2, :] = totals[1]


def fourth_kernel(shape, scaling, me_ref, frames, win, gain, dr_ref, dp_ref, dscales, late_small, *rest):
    slots, blocks, positions = shape
    slot_refs, (grad_frames, output, small, x_ref) = rest[:slots], rest[slots:]
    me = me_ref[0]
    size = slots * positions
    copy_blocks(shape, me, frames.now(), x_ref)
    for b in range(blocks):
        for k in range(slots):
            at = pl.multiple_of((me ^ k) * positions, positions)
            output[b, pl.ds(at, positions), :] = slot_refs[k][b * positions : (b + 1) * positions, :]
    grad_hidden = dot(dp_ref[...], win[...], 1, 1)
    result, grad_gain = norm_back(
        x_ref[...].astype(jnp.float32), dr_ref[...].astype(jnp.float32), grad_hidden, gain[...]
    )
    result = result.astype(jnp.bfloat16)
    for b in range(blocks):
        for k in range(slots):
            at = pl.multiple_of((me ^ k) * positions, positions)
            grad_frames[b, pl.ds(at, positions), :] = result[b * size + k * positions : b * size + (k + 1) * positions]
    fill_small(small, 0, scaling, [grad_gain, dscales[0:1, :], dscales[1:2, :]])
    half = late_small.shape[0]
    small[half:, :] = late_small[...]


def weights_kernel(plan, shards, scaling, me_ref, h_ref, dp_ref, g_ref, dr_ref, *rest):
    outs, (buffer,) = rest[: 2 * len(plan)], rest[2 * len(plan) :]
    me = me_ref[0]
    rows = outs[0].shape[1]
    width = dp_ref.shape[1]

    def place(index, column, size, offset_of):
        _, _, offsets = plan[index]
        kept, away = outs[2 * index], outs[2 * index + 1]
        for at, offset in enumerate(offsets):
            target = kept if at < shards // 2 else away
            top = pl.multiple_of(offset_of(me ^ offset), rows)
            target[at % (shards // 2), :, column : column + size] = buffer[pl.ds(top, rows), 0:size]

    count = buffer.shape[1]
    for index, (start, stop, _) in enumerate(plan):
        for at, size in column_chunks(max(min(stop, width) - start, 0), count):
            found = dot(h_ref[...], dp_ref[:, start + at : start + at + size], 0, 0) * scaling
            buffer[0 : h_ref.shape[1], 0:size] = found.astype(jnp.bfloat16)
            place(index, at, size, lambda r: r * rows)
    per = dr_ref.shape[1]
    pieces = g_ref.shape[1] // (shards * rows)
    for at, size in column_chunks(per, count):
        buffer[:, 0:size] = (dot(g_ref[...], dr_ref[:, at : at + size], 0, 0) * scaling).astype(jnp.bfloat16)
        for index, (start, stop, _) in enumerate(plan):
            for k in range(pieces):
                if start <= width + k * per + at < stop:
                    place(index, width + k * per + at - start, size, lambda r, k=k: (r * pieces + k) * rows)


def last_kernel(plans, small_ref, small_came, *rest):
    count = sum(len(plan) for plan in plans)
    parts, (grad_in, grad_out, gains, scales) = rest[: 2 * count], rest[2 * count :]
    width, per = grad_in.shape[2], grad_out.shape[2]
    rows = grad_in.shape[1]
    at = 0
    for unit, plan in enumerate(plans):
        for start, stop, _ in plan:
            kept, came = parts[2 * at], parts[2 * at + 1]
            at += 1
            total = kept[0].astype(jnp.float32) + came[0].astype(jnp.float32)
            low = min(stop, width)
            if start < low:
                grad_in[unit, :, start:low] = total[:, : low - start]
            for k in range(grad_out.shape[1] // rows):
                left, right = max(start, width + k * per), min(stop, width + (k + 1) * per)
                if left < right:
                    grad_out[unit, k * rows : (k + 1) * rows, left - width - k * per : right - width - k * per] = total[:, left - start : right - start]
    total = small_ref[...] + small_came[...]
    half = total.shape[0] // 2
    for unit in range(2):
        row = unit * half
        for column in range(0, gains.shape[1], 128):
            gains[unit : unit + 1, column : column + 128] = total[row : row + 1, :]
            row += 1
        for which in range(2):
            for column in range(0, scales.shape[2], 128):
                scales[unit, which : which + 1, column : column + 128] = total[row : row + 1, :]
                row += 1


VMEM = pltpu.MemorySpace.VMEM
SMEM = pltpu.MemorySpace.SMEM
HBM = pltpu.MemorySpace.HBM
LIMIT = 28 * 2**20


class Fetched:
    def __init__(self, source, unit, target, semaphore):
        self.copy = pltpu.make_async_copy(source if unit is None else source.at[unit], target, semaphore)
        self.copy.start()
        self.target = target
        self.shape = target.shape
        self.landed = False

    def now(self):
        if not self.landed:
            self.copy.wait()
            self.landed = True
        return self.target

    def __getitem__(self, index):
        return self.now()[index]


def run(body, ins, outs, scratch, flops):
    kinds = [len(v) if isinstance(v, tuple) else 0 for v in ins]
    fetched = [i for i, kind in enumerate(kinds) if kind == 2]
    specs = [pl.BlockSpec(memory_space=(VMEM, SMEM, HBM)[kind]) for kind in kinds]
    targets = []
    for i in fetched:
        array, unit = ins[i]
        targets.append(pltpu.VMEM(array.shape if unit is None else array.shape[1:], array.dtype))

    def kernel(*refs):
        refs = list(refs)
        spare = refs[len(refs) - len(fetched) - 1 :] if fetched else []
        refs = refs[: len(refs) - len(spare)]
        for k, i in enumerate(fetched):
            refs[i] = Fetched(refs[i], ins[i][1], spare[k], spare[-1].at[k])
        body(*refs)

    return pl.pallas_call(
        kernel,
        out_shape=[jax.ShapeDtypeStruct(s, d) for s, d in outs],
        in_specs=specs,
        out_specs=[pl.BlockSpec(memory_space=VMEM) for _ in outs],
        scratch_shapes=[pltpu.VMEM(s, d) for s, d in scratch]
        + targets
        + ([pltpu.SemaphoreType.DMA((len(fetched),))] if fetched else []),
        compiler_params=pltpu.CompilerParams(vmem_limit_bytes=LIMIT),
        cost_estimate=pl.CostEstimate(flops=flops, bytes_accessed=2**22, transcendentals=0),
    )(*[v[0] if isinstance(v, tuple) else v for v in ins])


def swapped(values, axis, mask):
    return lax.ppermute(values, axis, [(i, i ^ mask) for i in range(lax.axis_size(axis))])


def masks_of(size):
    count = size.bit_length() - 1
    masks = [1 << b for b in range(count)]
    if count >= 3:
        masks[-1] |= masks[-2]
    return masks


def rotated(masks, turn):
    first, *rest = masks
    turn %= max(len(rest), 1)
    return [first] + rest[turn:] + rest[:turn]


def offsets_of(masks):
    count = len(masks)
    offsets = []
    for place in range(1 << count):
        mask = 0
        for step in range(count):
            if place >> (count - 1 - step) & 1:
                mask ^= masks[step]
        offsets.append(mask)
    return offsets


def plan_of(width, turns):
    masks = masks_of(lax.axis_size("dp"))
    edges = [width * k // len(turns) // 128 * 128 for k in range(len(turns))] + [width]
    return [(edges[k], edges[k + 1], offsets_of(rotated(masks, turn))) for k, turn in enumerate(turns)]


class Chain:
    def __init__(self, kept, away, turn):
        self.steps = [("dp", m) for m in rotated(masks_of(lax.axis_size("dp")), turn)]
        self.halvings = len(self.steps)
        self.steps += [("seq", m) for m in masks_of(lax.axis_size("seq"))]
        self.kept, self.away = kept, away
        self.at = 0

    def send(self):
        self.came = swapped(self.away, *self.steps[self.at])

    def land(self):
        self.at += 1
        if self.done():
            return
        kept = self.kept.astype(jnp.float32)
        came = self.came.astype(jnp.float32)
        if self.at < self.halvings:
            half = kept.shape[0] // 2
            self.away = (kept[half:] + came[half:]).astype(jnp.bfloat16)
            self.kept = (kept[:half] + came[:half]).astype(jnp.bfloat16)
        else:
            self.away = self.kept = (kept + came).astype(jnp.bfloat16)

    def done(self):
        return self.at == len(self.steps)


LATE = (2,)
EARLY = (0, 1)


def unit_chains(plan, turns, scaling, me, hidden, grad_proj, gated, grad_result):
    size = lax.axis_size("dp")
    rows = hidden.shape[1] // size
    outs = [((size // 2, rows, stop - start), jnp.bfloat16) for start, stop, _ in plan for _ in range(2)]
    buffers = run(
        partial(weights_kernel, plan, size, scaling),
        [(me,), hidden, grad_proj, gated, grad_result],
        outs,
        [((max(hidden.shape[1], gated.shape[1]), 512), jnp.bfloat16)],
        2 * hidden.shape[0] * size * rows * plan[-1][1],
    )
    return [Chain(buffers[2 * k], buffers[2 * k + 1], turn) for k, turn in enumerate(turns)]


def tied(*values):
    return lax.optimization_barrier(values)


def on_device(frames, cotangent, weight_in, qk_scales, weight_out, gains):
    slots = lax.axis_size("seq")
    blocks = frames.shape[1] // BLOCK
    positions = BLOCK // slots
    shape = (slots, blocks, positions)
    count, width = frames.shape[1:]
    part = blocks * positions
    inner, half, shared = weight_in.shape[2], weight_out.shape[1], qk_scales.shape[2]
    tokens_all = frames.shape[0] * count * lax.axis_size("dp") * slots
    scaling = tokens_all ** (-0.5)
    me = lax.axis_index("seq").astype(jnp.int32).reshape(1)
    own = lax.axis_index("dp").astype(jnp.int32).reshape(1)
    flops = 2 * count * width * inner
    bf16, f32 = jnp.bfloat16, jnp.float32
    blocked = frames.reshape(blocks, BLOCK, width)
    turned = cotangent.reshape(blocks, BLOCK, width)
    lines = -(-(width + 2 * shared) // 1024) * 8
    slot_outs = [((part, width), bf16) for _ in range(slots)]

    def exchange(sends):
        return [swapped(sends[k], "seq", k) for k in range(1, slots)]

    pieces = turned.reshape(blocks, slots, positions, width)
    upstream = exchange(
        [
            lax.dynamic_index_in_dim(pieces, me[0] ^ k, 1, keepdims=False).reshape(part, width) if k else None
            for k in range(slots)
        ],
    )
    *first, hidden_first, proj_first = run(
        lambda me, x, wi, wo, sc, ga, *rest: first_kernel(
            shape, me, x, wi, wo, sc, Row(ga, 0), *rest
        ),
        [(me,), (blocked, None), (weight_in, 0), (weight_out, 0), (qk_scales, 0), (gains, None)],
        slot_outs + [((count, width), bf16), ((count, inner), bf16)],
        [((count, width), bf16), ((count, half), bf16), ((count, half), bf16)],
        2 * flops,
    )
    first_came = exchange(first)
    results = run(
        lambda me, dr, wi, wo, sc, ga, *rest: second_kernel(
            shape, slots * blocks, scaling, me, dr, wi, wo, sc, Row(ga, 1), *rest
        ),
        [(me,), (turned, None), (weight_in, 1), (weight_out, 1), (qk_scales, 1), (gains, None)]
        + [first[0]] + first_came + upstream,
        slot_outs + slot_outs
        + [
            ((count, width), bf16),
            ((count, inner), bf16),
            ((count, half), bf16),
            ((count, width), bf16),
            ((lines, 128), f32),
        ],
        [
            ((count, width), bf16),
            ((count, inner), f32),
            ((count, half), bf16),
            ((count, half), f32),
            ((count, count), f32),
            ((count, half), bf16),
        ],
        4 * flops,
    )
    second, back = results[:slots], results[slots : 2 * slots]
    hidden_second, dproj_second, gated_second, dresult_second, late_small = results[2 * slots :]
    back_came = exchange(back)
    columns = inner + half * width // hidden_second.shape[1]
    plans = [plan_of(columns, EARLY), plan_of(columns, LATE)]
    late = unit_chains(plans[1], LATE, scaling, own, hidden_second, dproj_second, gated_second, dresult_second)
    for chain in late:
        chain.send()
        chain.land()
    for chain in late:
        chain.send()
    *second_sends, back_came[0] = tied(*second[1:], back_came[0])
    second_came = exchange([None] + second_sends)
    dresult, dproj_first, gated_first, dscale_early = run(
        lambda wo, sc, *rest: third_kernel(shape, wo, sc, *rest),
        [(weight_out, 0), (qk_scales, 0), back[0]] + back_came + [proj_first],
        [((count, width), bf16), ((count, inner), bf16), ((count, half), bf16), ((2, shared), f32)],
        [((count, half), bf16), ((count, half), bf16)],
        2 * flops,
    )
    early = unit_chains(plans[0], EARLY, scaling, own, hidden_first, dproj_first, gated_first, dresult)
    grad_frames, output, small = run(
        lambda me, x, wi, ga, *rest: fourth_kernel(shape, scaling, me, x, wi, Row(ga, 0), *rest),
        [(me,), (blocked, None), (weight_in, 0), (gains, None), dresult, dproj_first, dscale_early, late_small]
        + [second[0]] + second_came,
        [((blocks, BLOCK, width), bf16), ((blocks, BLOCK, width), bf16), ((2 * lines, 128), f32)],
        [((count, width), bf16)],
        flops,
    )
    for chain in early:
        chain.send()
    for chain in late + early:
        chain.land()
    masks = [(a, m) for a in ("dp", "seq") for m in masks_of(lax.axis_size(a))]
    small_at = 0
    while small_at < len(masks) or not all(c.done() for c in early + late):
        live = [c for c in early + late if not c.done()]
        if small_at and small_at < len(masks):
            small, *aways = tied(small, *[c.away for c in live])
        else:
            aways = tied(*[c.away for c in live])
        for chain, away in zip(live, aways):
            chain.away = away
            chain.send()
        if small_at < len(masks):
            small_came = swapped(small, *masks[small_at])
            small_at += 1
            if small_at < len(masks):
                small = small + small_came
        for chain in live:
            chain.land()
    grad_in, grad_out, grad_gains, grad_scales = run(
        partial(last_kernel, plans),
        [small, small_came] + [v for c in early + late for v in (c.kept, c.came)],
        [
            ((2, weight_in.shape[1] // lax.axis_size("dp"), inner), f32),
            ((2, half // lax.axis_size("dp"), width), f32),
            (gains.shape, f32),
            (qk_scales.shape, f32),
        ],
        [],
        1000,
    )
    return (
        output.reshape(frames.shape),
        grad_frames.reshape(frames.shape),
        grad_in,
        grad_out,
        grad_gains,
        grad_scales,
    )


class Row:
    def __init__(self, fetched, row):
        self.fetched, self.row = fetched, row

    def __getitem__(self, index):
        return self.fetched.now()[self.row : self.row + 1, :]


def solution(mesh):
    in_specs = (P("dp", "seq", None), P("dp", "seq", None), P(), P(), P(), P())
    out_specs = (
        P("dp", "seq", None),
        P("dp", "seq", None),
        P(None, "dp", None),
        P(None, "dp", None),
        P(),
        P(),
    )

    return jax.shard_map(on_device, mesh=mesh, in_specs=in_specs, out_specs=out_specs, check_vma=False)
```

```python
from functools import partial

import jax
import jax.numpy as jnp
from jax import lax
from jax.experimental import pallas as pl
from jax.experimental.pallas import tpu as pltpu
from jax.sharding import PartitionSpec as P


BLOCK = 256


EPSILON = 1e-06


def sigmoid(values):
    return 0.5 * jnp.tanh(0.5 * values) + 0.5


def slope(values, sig):
    return sig * (1.0 + values * (1.0 - sig))


def dot(left, right, left_dim=1, right_dim=0):
    return lax.dot_general(
        left, right, (((left_dim,), (right_dim,)), ((), ())), preferred_element_type=jnp.float32
    )


def column_chunks(total, size):
    return [(at, min(size, total - at)) for at in range(0, total, size)]


CHUNK = 256


def norm_parts(values):
    scaling = lax.rsqrt(jnp.mean(values * values, axis=-1, keepdims=True) + EPSILON)
    return scaling, values * scaling


def norm_back(values, upstream, grad_hidden, gain_row):
    scaling, unit = norm_parts(values)
    grad_gain = jnp.sum(grad_hidden * unit, axis=0, keepdims=True)
    scaled = grad_hidden * gain_row
    mean = jnp.mean(scaled * unit, axis=-1, keepdims=True)
    return upstream + scaling * (scaled - unit * mean), grad_gain


def group_mask(rows, columns, positions):
    left = lax.broadcasted_iota(jnp.int32, (rows, columns), 0)
    right = lax.broadcasted_iota(jnp.int32, (rows, columns), 1)
    return lax.rem(left, positions) == lax.rem(right, positions)


def scores_of(query, keyed, positions):
    found = jnp.maximum(dot(query, keyed, 1, 1) * query.shape[1] ** (-0.5), 0.0)
    if positions is not None:
        found = jnp.where(group_mask(found.shape[0], found.shape[1], positions), found, 0.0)
    return found


def forward_core(x_ref, h_ref, p_ref, v_ref, o_ref, g_ref, r_ref, win, wout, scales, gain, sets, positions, length):
    half = wout.shape[0]
    values = x_ref[...].astype(jnp.float32)
    h_ref[...] = (norm_parts(values)[1] * gain[...]).astype(jnp.bfloat16)
    shared = dot(h_ref[...], win[:, 2 * half :])
    p_ref[:, 2 * half :] = shared.astype(p_ref.dtype)
    active = shared * sigmoid(shared)
    query = (active * scales[0:1, :]).astype(jnp.bfloat16)
    keyed = (active * scales[1:2, :]).astype(jnp.bfloat16)
    weights = []
    for start, stop in sets:
        found = scores_of(query[start:stop], keyed[start:stop], positions)
        if r_ref is not None:
            r_ref[start:stop, :] = found
        weights.append((found * found * (1.0 / length)).astype(jnp.bfloat16))
    for at, size in column_chunks(half, CHUNK):
        value = dot(h_ref[...], win[:, half + at : half + at + size])
        p_ref[:, half + at : half + at + size] = value.astype(p_ref.dtype)
        v_ref[:, at : at + size] = (value * sigmoid(value)).astype(jnp.bfloat16)
        gate = dot(h_ref[...], win[:, at : at + size])
        p_ref[:, at : at + size] = gate.astype(p_ref.dtype)
        gate = gate * sigmoid(gate)
        for (start, stop), weight in zip(sets, weights):
            mixed = dot(weight, v_ref[start:stop, at : at + size])
            if o_ref is not None:
                o_ref[start:stop, at : at + size] = mixed
            g_ref[start:stop, at : at + size] = (gate[start:stop] * mixed).astype(jnp.bfloat16)
    return values + dot(g_ref[...], wout[...])


def backward_core(dr_ref, p_ref, v_ref, o_ref, g_ref, r_ref, do_ref, dp_ref, wout, scales, sets, positions, length):
    half = wout.shape[0]
    width = scales.shape[1]
    again = o_ref is None
    shared = p_ref[:, 2 * half :].astype(jnp.float32)
    shared_sig = sigmoid(shared)
    active = shared * shared_sig
    query = (active * scales[0:1, :]).astype(jnp.bfloat16)
    keyed = (active * scales[1:2, :]).astype(jnp.bfloat16)
    found, weights = [], []
    for start, stop in sets:
        if again:
            found.append(scores_of(query[start:stop], keyed[start:stop], positions))
        else:
            found.append(r_ref[start:stop, :])
        weights.append((found[-1] * found[-1] * (1.0 / length)).astype(jnp.bfloat16))
    grad_weights = [None for _ in sets]
    for at, size in column_chunks(half, CHUNK):
        here = slice(at, at + size)
        value_here = slice(half + at, half + at + size)
        value = p_ref[:, value_here].astype(jnp.float32)
        value_sig = sigmoid(value)
        if again:
            v_ref[:, here] = (value * value_sig).astype(jnp.bfloat16)
        grad_gated = dot(dr_ref[...], wout[here, :], 1, 1).astype(jnp.bfloat16).astype(jnp.float32)
        gate = p_ref[:, here].astype(jnp.float32)
        gate_sig = sigmoid(gate)
        gated = gate * gate_sig
        do_ref[:, here] = (grad_gated * gated).astype(jnp.bfloat16)
        outer = grad_gated * slope(gate, gate_sig)
        inner = slope(value, value_sig)
        for index, (start, stop) in enumerate(sets):
            if again:
                mixed = dot(weights[index], v_ref[start:stop, here])
                g_ref[start:stop, here] = (gated[start:stop] * mixed).astype(jnp.bfloat16)
            else:
                mixed = o_ref[start:stop, here]
            dp_ref[start:stop, here] = (outer[start:stop] * mixed).astype(jnp.bfloat16)
            grad_value = dot(weights[index], do_ref[start:stop, here], 0, 0)
            grad_value = grad_value.astype(jnp.bfloat16).astype(jnp.float32)
            dp_ref[start:stop, value_here] = (grad_value * inner[start:stop]).astype(jnp.bfloat16)
    totals = [jnp.zeros((1, width), jnp.float32), jnp.zeros((1, width), jnp.float32)]
    for index, (start, stop) in enumerate(sets):
        grad_weight = dot(do_ref[start:stop, :], v_ref[start:stop, :], 1, 1)
        grad_weight = grad_weight.astype(jnp.bfloat16).astype(jnp.float32)
        grad_score = grad_weight * found[index] * (2.0 / length * width ** (-0.5))
        if positions is not None:
            grad_score = jnp.where(
                group_mask(grad_score.shape[0], grad_score.shape[1], positions), grad_score, 0.0
            )
        grad_score = grad_score.astype(jnp.bfloat16)
        part = active[start:stop]
        grad_query = dot(grad_score, keyed[start:stop]).astype(jnp.bfloat16).astype(jnp.float32)
        grad_keyed = dot(grad_score, query[start:stop], 0, 0).astype(jnp.bfloat16).astype(jnp.float32)
        totals[0] += jnp.sum(grad_query * part, axis=0, keepdims=True)
        totals[1] += jnp.sum(grad_keyed * part, axis=0, keepdims=True)
        grad_shared = grad_query * scales[0:1, :] + grad_keyed * scales[1:2, :]
        grad_shared = grad_shared * slope(shared[start:stop], shared_sig[start:stop])
        dp_ref[start:stop, 2 * half :] = grad_shared.astype(jnp.bfloat16)
    return totals


def copy_blocks(shape, me, source, target):
    slots, blocks, positions = shape
    size = slots * positions
    for b in range(blocks):
        for k in range(slots):
            at = pl.multiple_of((me ^ k) * positions, positions)
            target[b * size + k * positions : b * size + (k + 1) * positions, :] = source[b, pl.ds(at, positions), :]


def first_kernel(shape, me_ref, frames, win, wout, scales, gain, *rest):
    slots, blocks, positions = shape
    sends, (h_ref, p_ref, x_ref, v_ref, g_ref) = rest[:slots], rest[slots:]
    size = slots * positions
    copy_blocks(shape, me_ref[0], frames.now(), x_ref)
    sets = [(b * size, (b + 1) * size) for b in range(blocks)]
    result = forward_core(
        x_ref, h_ref, p_ref, v_ref, None, g_ref, None, win, wout, scales, gain, sets, None, size
    ).astype(jnp.bfloat16)
    for b in range(blocks):
        for k in range(slots):
            sends[k][b * positions : (b + 1) * positions, :] = result[b * size + k * positions : b * size + (k + 1) * positions]


def second_kernel(shape, length, scaling, me_ref, cotangent, win, wout, scales, gain, *rest):
    slots, blocks, positions = shape
    part = blocks * positions
    xs, drs, rest = rest[:slots], rest[slots : 2 * slots - 1], rest[2 * slots - 1 :]
    seconds, backs, rest = rest[:slots], rest[slots : 2 * slots], rest[2 * slots :]
    h_ref, dp_ref, g_ref, dr_ref, small, x_ref, p_ref, v_ref, o_ref, r_ref, do_ref = rest
    at = pl.multiple_of(me_ref[0] * positions, positions)
    for k in range(slots):
        x_ref[k * part : (k + 1) * part, :] = xs[k][...]
        if k:
            dr_ref[k * part : (k + 1) * part, :] = drs[k - 1][...]
    for b in range(blocks):
        dr_ref[b * positions : (b + 1) * positions, :] = cotangent.now()[b, pl.ds(at, positions), :]
    sets = [(0, x_ref.shape[0])]
    result = forward_core(
        x_ref, h_ref, p_ref, v_ref, o_ref, g_ref, r_ref, win, wout, scales, gain, sets, positions, length
    ).astype(jnp.bfloat16)
    for k in range(slots):
        seconds[k][...] = result[k * part : (k + 1) * part]
    totals = backward_core(
        dr_ref, p_ref, v_ref, o_ref, g_ref, r_ref, do_ref, dp_ref, wout, scales, sets, positions, length
    )
    grad_hidden = dot(dp_ref[...], win[...], 1, 1)
    result, grad_gain = norm_back(
        x_ref[...].astype(jnp.float32), dr_ref[...].astype(jnp.float32), grad_hidden, gain[...]
    )
    result = result.astype(jnp.bfloat16)
    for k in range(slots):
        backs[k][...] = result[k * part : (k + 1) * part]
    fill_small(small, 0, scaling, [grad_gain] + totals)


def fill_small(small, start, scaling, values):
    row = start
    for value in values:
        for at in range(0, value.shape[1], 128):
            small[row : row + 1, :] = value[:, at : at + 128] * scaling
            row += 1
    while row % 8:
        small[row : row + 1, :] = jnp.zeros((1, 128), jnp.float32)
        row += 1


def third_kernel(shape, wout, scales, *rest):
    slots, blocks, positions = shape
    size = slots * positions
    slot_refs, (p_ref, dr_ref, dp_ref, g_ref, dscales, v_ref, do_ref) = rest[:slots], rest[slots:]
    for b in range(blocks):
        for k in range(slots):
            dr_ref[b * size + k * positions : b * size + (k + 1) * positions, :] = slot_refs[k][b * positions : (b + 1) * positions, :]
    sets = [(b * size, (b + 1) * size) for b in range(blocks)]
    totals = backward_core(
        dr_ref, p_ref, v_ref, None, g_ref, None, do_ref, dp_ref, wout, scales, sets, None, size
    )
    dscales[0:1, :] = totals[0]
    dscales[1:2, :] = totals[1]


def fourth_kernel(shape, scaling, me_ref, frames, win, gain, dr_ref, dp_ref, dscales, late_small, *rest):
    slots, blocks, positions = shape
    slot_refs, (grad_frames, output, small, x_ref) = rest[:slots], rest[slots:]
    me = me_ref[0]
    size = slots * positions
    copy_blocks(shape, me, frames.now(), x_ref)
    for b in range(blocks):
        for k in range(slots):
            at = pl.multiple_of((me ^ k) * positions, positions)
            output[b, pl.ds(at, positions), :] = slot_refs[k][b * positions : (b + 1) * positions, :]
    grad_hidden = dot(dp_ref[...], win[...], 1, 1)
    result, grad_gain = norm_back(
        x_ref[...].astype(jnp.float32), dr_ref[...].astype(jnp.float32), grad_hidden, gain[...]
    )
    result = result.astype(jnp.bfloat16)
    for b in range(blocks):
        for k in range(slots):
            at = pl.multiple_of((me ^ k) * positions, positions)
            grad_frames[b, pl.ds(at, positions), :] = result[b * size + k * positions : b * size + (k + 1) * positions]
    fill_small(small, 0, scaling, [grad_gain, dscales[0:1, :], dscales[1:2, :]])
    half = late_small.shape[0]
    small[half:, :] = late_small[...]


def weights_kernel(plan, shards, scaling, me_ref, h_ref, dp_ref, g_ref, dr_ref, *rest):
    outs, (buffer,) = rest[: 2 * len(plan)], rest[2 * len(plan) :]
    me = me_ref[0]
    rows = outs[0].shape[1]
    width = dp_ref.shape[1]

    def place(index, column, size, offset_of):
        _, _, offsets = plan[index]
        kept, away = outs[2 * index], outs[2 * index + 1]
        for at, offset in enumerate(offsets):
            target = kept if at < shards // 2 else away
            top = pl.multiple_of(offset_of(me ^ offset), rows)
            target[at % (shards // 2), :, column : column + size] = buffer[pl.ds(top, rows), 0:size]

    count = buffer.shape[1]
    for index, (start, stop, _) in enumerate(plan):
        for at, size in column_chunks(max(min(stop, width) - start, 0), count):
            found = dot(h_ref[...], dp_ref[:, start + at : start + at + size], 0, 0) * scaling
            buffer[0 : h_ref.shape[1], 0:size] = found.astype(jnp.bfloat16)
            place(index, at, size, lambda r: r * rows)
    per = dr_ref.shape[1]
    pieces = g_ref.shape[1] // (shards * rows)
    for at, size in column_chunks(per, count):
        buffer[:, 0:size] = (dot(g_ref[...], dr_ref[:, at : at + size], 0, 0) * scaling).astype(jnp.bfloat16)
        for index, (start, stop, _) in enumerate(plan):
            for k in range(pieces):
                if start <= width + k * per + at < stop:
                    place(index, width + k * per + at - start, size, lambda r, k=k: (r * pieces + k) * rows)


def last_kernel(plans, small_ref, small_came, *rest):
    count = sum(len(plan) for plan in plans)
    parts, (grad_in, grad_out, gains, scales) = rest[: 2 * count], rest[2 * count :]
    width, per = grad_in.shape[2], grad_out.shape[2]
    rows = grad_in.shape[1]
    at = 0
    for unit, plan in enumerate(plans):
        for start, stop, _ in plan:
            kept, came = parts[2 * at], parts[2 * at + 1]
            at += 1
            total = kept[0].astype(jnp.float32) + came[0].astype(jnp.float32)
            low = min(stop, width)
            if start < low:
                grad_in[unit, :, start:low] = total[:, : low - start]
            for k in range(grad_out.shape[1] // rows):
                left, right = max(start, width + k * per), min(stop, width + (k + 1) * per)
                if left < right:
                    grad_out[unit, k * rows : (k + 1) * rows, left - width - k * per : right - width - k * per] = total[:, left - start : right - start]
    total = small_ref[...] + small_came[...]
    half = total.shape[0] // 2
    for unit in range(2):
        row = unit * half
        for column in range(0, gains.shape[1], 128):
            gains[unit : unit + 1, column : column + 128] = total[row : row + 1, :]
            row += 1
        for which in range(2):
            for column in range(0, scales.shape[2], 128):
                scales[unit, which : which + 1, column : column + 128] = total[row : row + 1, :]
                row += 1


VMEM = pltpu.MemorySpace.VMEM
SMEM = pltpu.MemorySpace.SMEM
HBM = pltpu.MemorySpace.HBM
LIMITS = {"first": 62, "second": 48, "late": 48, "third": 48, "early": 48, "fourth": 48, "last": 28}


class Fetched:
    def __init__(self, source, unit, target, semaphore):
        self.copy = pltpu.make_async_copy(source if unit is None else source.at[unit], target, semaphore)
        self.copy.start()
        self.target = target
        self.shape = target.shape
        self.landed = False

    def now(self):
        if not self.landed:
            self.copy.wait()
            self.landed = True
        return self.target

    def __getitem__(self, index):
        return self.now()[index]


def run(name, body, ins, outs, scratch, flops):
    kinds = [len(v) if isinstance(v, tuple) else 0 for v in ins]
    fetched = [i for i, kind in enumerate(kinds) if kind == 2]
    specs = [pl.BlockSpec(memory_space=(VMEM, SMEM, HBM)[kind]) for kind in kinds]
    targets = []
    for i in fetched:
        array, unit = ins[i]
        targets.append(pltpu.VMEM(array.shape if unit is None else array.shape[1:], array.dtype))

    def kernel(*refs):
        refs = list(refs)
        spare = refs[len(refs) - len(fetched) - 1 :] if fetched else []
        refs = refs[: len(refs) - len(spare)]
        for k, i in enumerate(fetched):
            refs[i] = Fetched(refs[i], ins[i][1], spare[k], spare[-1].at[k])
        body(*refs)

    return pl.pallas_call(
        kernel,
        out_shape=[jax.ShapeDtypeStruct(s, d) for s, d in outs],
        in_specs=specs,
        out_specs=[pl.BlockSpec(memory_space=VMEM) for _ in outs],
        scratch_shapes=[pltpu.VMEM(s, d) for s, d in scratch]
        + targets
        + ([pltpu.SemaphoreType.DMA((len(fetched),))] if fetched else []),
        compiler_params=pltpu.CompilerParams(vmem_limit_bytes=LIMITS[name] * 2**20),
        cost_estimate=pl.CostEstimate(flops=flops, bytes_accessed=2**22, transcendentals=0),
    )(*[v[0] if isinstance(v, tuple) else v for v in ins])


def swapped(values, axis, mask):
    return lax.ppermute(values, axis, [(i, i ^ mask) for i in range(lax.axis_size(axis))])


def masks_of(size):
    return [1 << b for b in range(size.bit_length() - 1)]


def rotated(masks, turn):
    masks = list(masks)
    if turn and len(masks) > 2:
        masks[1], masks[2] = masks[2], masks[1]
    return masks


def offsets_of(masks):
    count = len(masks)
    offsets = []
    for place in range(1 << count):
        mask = 0
        for step in range(count):
            if place >> (count - 1 - step) & 1:
                mask ^= masks[step]
        offsets.append(mask)
    return offsets


def plan_of(width, turns):
    masks = masks_of(lax.axis_size("dp"))
    edges = [width * k // len(turns) // 128 * 128 for k in range(len(turns))] + [width]
    return [(edges[k], edges[k + 1], offsets_of(rotated(masks, turn))) for k, turn in enumerate(turns)]


class Chain:
    def __init__(self, kept, away, turn):
        self.steps = [("dp", m) for m in rotated(masks_of(lax.axis_size("dp")), turn)]
        self.halvings = len(self.steps)
        self.steps += [("seq", m) for m in masks_of(lax.axis_size("seq"))]
        self.kept, self.away = kept, away
        self.at = 0

    def send(self):
        self.came = swapped(self.away, *self.steps[self.at])

    def land(self):
        self.at += 1
        if self.done():
            return
        if self.at < self.halvings:
            half = self.kept.shape[0] // 2
            self.away = self.kept[half:] + self.came[half:]
            self.kept = self.kept[:half] + self.came[:half]
        else:
            self.away = self.kept = self.kept + self.came

    def done(self):
        return self.at == len(self.steps)


LATE = (0, 1)
EARLY = (0, 1)


def unit_chains(name, plan, turns, scaling, me, hidden, grad_proj, gated, grad_result):
    size = lax.axis_size("dp")
    rows = hidden.shape[1] // size
    outs = [((size // 2, rows, stop - start), jnp.bfloat16) for start, stop, _ in plan for _ in range(2)]
    buffers = run(
        name,
        partial(weights_kernel, plan, size, scaling),
        [(me,), hidden, grad_proj, gated, grad_result],
        outs,
        [((max(hidden.shape[1], gated.shape[1]), 512), jnp.bfloat16)],
        2 * hidden.shape[0] * size * rows * plan[-1][1],
    )
    return [Chain(buffers[2 * k], buffers[2 * k + 1], turn) for k, turn in enumerate(turns)]


def tied(*values):
    return lax.optimization_barrier(values)


def on_device(frames, cotangent, weight_in, qk_scales, weight_out, gains):
    slots = lax.axis_size("seq")
    blocks = frames.shape[1] // BLOCK
    positions = BLOCK // slots
    shape = (slots, blocks, positions)
    count, width = frames.shape[1:]
    part = blocks * positions
    inner, half, shared = weight_in.shape[2], weight_out.shape[1], qk_scales.shape[2]
    tokens_all = frames.shape[0] * count * lax.axis_size("dp") * slots
    scaling = tokens_all ** (-0.5)
    me = lax.axis_index("seq").astype(jnp.int32).reshape(1)
    own = lax.axis_index("dp").astype(jnp.int32).reshape(1)
    flops = 2 * count * width * inner
    bf16, f32 = jnp.bfloat16, jnp.float32
    blocked = frames.reshape(blocks, BLOCK, width)
    turned = cotangent.reshape(blocks, BLOCK, width)
    lines = -(-(width + 2 * shared) // 1024) * 8
    slot_outs = [((part, width), bf16) for _ in range(slots)]

    def exchange(sends):
        return [swapped(sends[k], "seq", k) for k in range(1, slots)]

    pieces = turned.reshape(blocks, slots, positions, width)
    upstream = exchange(
        [
            lax.dynamic_index_in_dim(pieces, me[0] ^ k, 1, keepdims=False).reshape(part, width) if k else None
            for k in range(slots)
        ],
    )
    *first, hidden_first, proj_first = run(
        "first",
        lambda me, x, wi, wo, sc, ga, *rest: first_kernel(
            shape, me, x, wi, wo, sc, Row(ga, 0), *rest
        ),
        [(me,), (blocked, None), (weight_in, 0), (weight_out, 0), (qk_scales, 0), (gains, None)],
        slot_outs + [((count, width), bf16), ((count, inner), bf16)],
        [((count, width), bf16), ((count, half), bf16), ((count, half), bf16)],
        2 * flops,
    )
    first_came = exchange(first)
    results = run(
        "second",
        lambda me, dr, wi, wo, sc, ga, *rest: second_kernel(
            shape, slots * blocks, scaling, me, dr, wi, wo, sc, Row(ga, 1), *rest
        ),
        [(me,), (turned, None), (weight_in, 1), (weight_out, 1), (qk_scales, 1), (gains, None)]
        + [first[0]] + first_came + upstream,
        slot_outs + slot_outs
        + [
            ((count, width), bf16),
            ((count, inner), bf16),
            ((count, half), bf16),
            ((count, width), bf16),
            ((lines, 128), f32),
        ],
        [
            ((count, width), bf16),
            ((count, inner), f32),
            ((count, half), bf16),
            ((count, half), f32),
            ((count, count), f32),
            ((count, half), bf16),
        ],
        4 * flops,
    )
    second, back = results[:slots], results[slots : 2 * slots]
    hidden_second, dproj_second, gated_second, dresult_second, late_small = results[2 * slots :]
    back_came = exchange(back)
    columns = inner + half * width // hidden_second.shape[1]
    plans = [plan_of(columns, EARLY), plan_of(columns, LATE)]
    late = unit_chains(
        "late", plans[1], LATE, scaling, own, hidden_second, dproj_second, gated_second, dresult_second
    )
    for chain in late:
        chain.send()
        chain.land()
    for chain in late:
        chain.send()
    *second_sends, back_came[0] = tied(*second[1:], back_came[0])
    second_came = exchange([None] + second_sends)
    dresult, dproj_first, gated_first, dscale_early = run(
        "third",
        lambda wo, sc, *rest: third_kernel(shape, wo, sc, *rest),
        [(weight_out, 0), (qk_scales, 0), back[0]] + back_came + [proj_first],
        [((count, width), bf16), ((count, inner), bf16), ((count, half), bf16), ((2, shared), f32)],
        [((count, half), bf16), ((count, half), bf16)],
        2 * flops,
    )
    early = unit_chains(
        "early", plans[0], EARLY, scaling, own, hidden_first, dproj_first, gated_first, dresult
    )
    grad_frames, output, small = run(
        "fourth",
        lambda me, x, wi, ga, *rest: fourth_kernel(shape, scaling, me, x, wi, Row(ga, 0), *rest),
        [(me,), (blocked, None), (weight_in, 0), (gains, None), dresult, dproj_first, dscale_early, late_small]
        + [second[0]] + second_came,
        [((blocks, BLOCK, width), bf16), ((blocks, BLOCK, width), bf16), ((2 * lines, 128), f32)],
        [((count, width), bf16)],
        flops,
    )
    for chain in early:
        chain.send()
    for chain in late + early:
        chain.land()
    masks = [(a, m) for a in ("dp", "seq") for m in masks_of(lax.axis_size(a))]
    small_at = 0
    while small_at < len(masks) or not all(c.done() for c in early + late):
        live = [c for c in early + late if not c.done()]
        if small_at and small_at < len(masks):
            small, *aways = tied(small, *[c.away for c in live])
        else:
            aways = tied(*[c.away for c in live])
        for chain, away in zip(live, aways):
            chain.away = away
            chain.send()
        if small_at < len(masks):
            small_came = swapped(small, *masks[small_at])
            small_at += 1
            if small_at < len(masks):
                small = small + small_came
        for chain in live:
            chain.land()
    grad_in, grad_out, grad_gains, grad_scales = run(
        "last",
        partial(last_kernel, plans),
        [small, small_came] + [v for c in early + late for v in (c.kept, c.came)],
        [
            ((2, weight_in.shape[1] // lax.axis_size("dp"), inner), f32),
            ((2, half // lax.axis_size("dp"), width), f32),
            (gains.shape, f32),
            (qk_scales.shape, f32),
        ],
        [],
        1000,
    )
    return (
        output.reshape(frames.shape),
        grad_frames.reshape(frames.shape),
        grad_in,
        grad_out,
        grad_gains,
        grad_scales,
    )


class Row:
    def __init__(self, fetched, row):
        self.fetched, self.row = fetched, row

    def __getitem__(self, index):
        return self.fetched.now()[self.row : self.row + 1, :]


def solution(mesh):
    in_specs = (P("dp", "seq", None), P("dp", "seq", None), P(), P(), P(), P())
    out_specs = (
        P("dp", "seq", None),
        P("dp", "seq", None),
        P(None, "dp", None),
        P(None, "dp", None),
        P(),
        P(),
    )

    return jax.shard_map(on_device, mesh=mesh, in_specs=in_specs, out_specs=out_specs, check_vma=False)
```
